32 devices in a mesh: owner: 4 (over y, x), rows: 8 (over z, core).
Axes of the slice: x: 2, y: 2, z: 4, core: 2. Of those that a mesh axis runs over, the one named last changes fastest.
Arguments:
- train_gate: float32 [128, 2048, 768], P('owner', 'rows'), may hold values from -0.1875 to 0.1875
- other_gate: bfloat16 [128, 2048, 768], P('owner', 'rows'), may hold values from -0.0625 to 0.0625
- train_up: float32 [128, 2048, 768], P('owner', 'rows'), may hold values from -0.1875 to 0.1875
- other_up: bfloat16 [128, 2048, 768], P('owner', 'rows'), may hold values from -0.0625 to 0.0625
- router_weight: float32 [2048, 128], P('rows', 'owner'), may hold values from -0.125 to 0.125
- router_gain: float32 [2048], P('rows'), may hold values from 0.25 to 1.75
Outputs:
- ready_gate: bfloat16 [128, 2048, 768], P(('owner', 'rows'))
- ready_up: bfloat16 [128, 2048, 768], P(('owner', 'rows'))
- scale_gate: float32 [128, 768], P(('owner', 'rows'))
- scale_up: float32 [128, 768], P(('owner', 'rows'))
- serve_router: bfloat16 [2048, 128], replicated
The draws below stay inside these ranges and needn't reach their ends.
All inputs are finite; a program needn't handle non-finite values. Where the reference program divides by a largest or mean magnitude, that divisor is 1e-20 or more.
Results may differ from the reference program's by a relative error of at most 0.001.
Values may be sent and summed in bfloat16 or wider, within the bound.
A program may use at most 192 MiB of HBM per device.

```python
import jax
import jax.numpy as jnp

EXPERTS = 128
D_MODEL = 2048
D_EXPERT = 768


def strengthened(entries, stream_key, source, target, shards_of, factor):
    def block_of(position):
        return (jnp.arange(entries.shape[position]) // (entries.shape[position] // shards_of)).reshape((-1,) + (1,) * (entries.ndim - 1 - position))

    first = jax.random.permutation(stream_key, shards_of)[block_of(target)]
    other_side = (block_of(target) + shards_of // 2) % shards_of
    return jnp.where((block_of(source) == first) | (block_of(source) == other_side), factor * entries, entries)


def steps_of(rng, extent, split, least, largest):
    loudness, own = 1.0, jax.random.fold_in(rng, 6)
    for axis_at, blocks in split:
        heights = jnp.exp(jax.random.uniform(jax.random.fold_in(own, axis_at), (blocks,), jnp.float32, least / len(split), largest / len(split)))
        loudness = loudness * jnp.repeat(heights, extent[axis_at] // blocks).reshape([-1 if axis == axis_at else 1 for axis in range(len(extent))])
    return loudness


def noise(own_key, shape, width, reach, pieces=(), dtype=jnp.bfloat16):
    drawn = width * jax.random.normal(own_key, shape, jnp.float32)
    if pieces:
        drawn = drawn * steps_of(own_key, shape, pieces, -0.22, 0.18)
    return jnp.clip(drawn, -reach, reach).astype(dtype)


def noise_with(own_key, shape, width, most, split, heavy, dtype=jnp.bfloat16):
    entries = width * jax.random.normal(own_key, shape, jnp.float32)
    if split:
        entries = entries * steps_of(own_key, shape, split, -0.22, 0.18)
    return jnp.clip(strengthened(entries, jax.random.fold_in(own_key, 3), *heavy), -most, most).astype(dtype)


def setup_inputs(seed: int = 0) -> dict:
    key_list = jax.random.split(jax.random.key(seed), 7)
    return {
        "train_gate": noise_with(key_list[0], (EXPERTS, D_MODEL, D_EXPERT), D_MODEL ** -0.5, 0.1875, ((0, 4), (1, 8)), (1, 2, 8, 2.0), jnp.float32),
        "other_gate": noise(key_list[1], (EXPERTS, D_MODEL, D_EXPERT), (D_MODEL * 4) ** -0.5, 0.0625, ((0, 4), (1, 8))),
        "train_up": noise_with(key_list[2], (EXPERTS, D_MODEL, D_EXPERT), D_MODEL ** -0.5, 0.1875, ((0, 4), (1, 8)), (1, 2, 8, 2.0), jnp.float32),
        "other_up": noise(key_list[3], (EXPERTS, D_MODEL, D_EXPERT), (D_MODEL * 4) ** -0.5, 0.0625, ((0, 4), (1, 8))),
        "router_weight": noise(key_list[4], (D_MODEL, EXPERTS), D_MODEL ** -0.5, 0.125, ((0, 8), (1, 4)), jnp.float32),
        "router_gain": jnp.clip(1.0 + 0.15 * jax.random.normal(key_list[5], (D_MODEL,), jnp.float32), 0.25, 1.75),
    }


def reference(train_gate, other_gate, train_up, other_up, router_weight, router_gain):
    latest_gate = train_gate + other_gate.astype(jnp.float32)
    latest_up = train_up + other_up.astype(jnp.float32)
    scale_gate = jnp.max(jnp.abs(latest_gate), axis=1)
    ready_gate = (latest_gate / jnp.expand_dims(scale_gate, 1)).astype(jnp.bfloat16)
    scale_up = jnp.max(jnp.abs(latest_up), axis=1)
    ready_up = (latest_up / jnp.expand_dims(scale_up, 1)).astype(jnp.bfloat16)
    serve_router = (router_weight * router_gain[:, None]).astype(jnp.bfloat16)
    return ready_gate, ready_up, scale_gate, scale_up, serve_router
```

```python
import functools

import jax
import jax.numpy as jnp
from jax import lax
from jax.experimental import pallas as pl
from jax.experimental.pallas import tpu as pltpu
from jax.sharding import PartitionSpec as P

F32, BF16 = jnp.float32, jnp.bfloat16
CHUNK = 32


def flipped(me, k, n):
    out, bit = 0, 1
    while bit < n:
        out = out + ((me // bit + k // bit) % 2) * bit
        bit *= 2
    return out


def kernel(n, owners, each, train_gate, other_gate, train_up, other_up, part_router,
           ready_gate, ready_up, scales, router,
           wide, narrow, send, mx, rx, full,
           load_sem, send_sem, recv_sem, own_sem, mx_sem, rx_sem, fl_sem, fr_sem,
           rt_send, rt_recv, ro_send, ro_recv, rt_own):
    me, owner = lax.axis_index("rows"), lax.axis_index("owner")
    rows = wide.shape[2]
    units = 2 * each
    trains, others, readies = (train_gate, train_up), (other_gate, other_up), (ready_gate, ready_up)

    def loads(step):
        unit, slot = step % units, step % 2
        kind, j = unit // each, unit % each
        return (
            pltpu.make_async_copy(trains[kind].at[:, j], wide.at[slot], load_sem.at[slot, 0]),
            pltpu.make_async_copy(others[kind].at[:, j], narrow.at[slot], load_sem.at[slot, 1]),
        )

    def start(step):
        if step < 2 * units:
            for copy in loads(step):
                copy.start()

    def remote(src, dst, s, r, **where):
        return pltpu.make_async_remote_copy(
            src_ref=src, dst_ref=dst, send_sem=s, recv_sem=r, device_id=where,
            device_id_type=pl.DeviceIdType.MESH,
        )

    start(0)
    start(1)
    barrier = pltpu.get_barrier_semaphore()
    for k in range(1, n):
        pl.semaphore_signal(barrier, inc=1, device_id={"rows": (me + k) % n},
                            device_id_type=pl.DeviceIdType.MESH)
    for k in range(1, owners):
        pl.semaphore_signal(barrier, inc=1, device_id={"owner": (owner + k) % owners},
                            device_id_type=pl.DeviceIdType.MESH)
    pl.semaphore_wait(barrier, n - 1 + owners - 1)

    def router_rows(k):
        return remote(part_router, router.at[owner, me], rt_send.at[k], rt_recv.at[k],
                      rows=(me + k) % n)

    def router_owners(k):
        return remote(router.at[owner], router.at[owner], ro_send.at[k], ro_recv.at[k],
                      owner=(owner + k) % owners)

    own_router = pltpu.make_async_copy(part_router, router.at[owner, me], rt_own)
    own_router.start()
    for k in range(1, n):
        router_rows(k).start()

    for unit in range(units):
        slot = unit % 2
        for copy in loads(unit):
            copy.wait()

        def largest(d, _, slot=slot, unit=unit):
            acc = None
            for i in range(rows // CHUNK):
                x = wide[slot, d, i * CHUNK:(i + 1) * CHUNK, :]
                y = narrow[slot, d, i * CHUNK:(i + 1) * CHUNK, :].astype(F32)
                a = jnp.abs(x + y)
                acc = a if acc is None else jnp.maximum(acc, a)
            mx[d, unit:unit + 1, :] = jnp.max(acc, axis=0, keepdims=True)
            return 0

        lax.fori_loop(0, n, largest, 0)
        start(unit + 2)

    def to_owner(k):
        d = (me + k) % n
        return remote(mx.at[d], rx.at[me], mx_sem.at[k], rx_sem.at[k], rows=d)

    def to_all(k):
        return remote(scales, full.at[me], fl_sem.at[k], fr_sem.at[k], rows=(me + k) % n)

    for k in range(1, n):
        to_owner(k).start()
    rx[me] = mx[me]
    for k in range(1, n):
        to_owner(k).wait()
    total = rx[0]
    for d in range(1, n):
        total = jnp.maximum(total, rx[d])
    scales[...] = total
    full[me] = total
    for k in range(1, n):
        to_all(k).start()
    own_router.wait()
    for k in range(1, n):
        router_rows(k).wait()
    for k in range(1, owners):
        router_owners(k).start()
    for k in range(1, n):
        to_all(k).wait()

    far, near = list(range(n // 2, n)), list(range(2, n // 2))
    side = me % 2

    def dest(p):
        a, b, c = len(far), len(near), n // 2
        in_far = jnp.where(side == 0, p < a, jnp.logical_and(p >= b, p < a + b))
        at_far = p - side * b
        at_near = p - (1 - side) * a
        k = jnp.where(p == n - 2, 1, jnp.where(in_far, c + at_far, 2 + at_near))
        return flipped(me, k, n)

    def data(unit, p, d):
        kind, j = unit // each, unit % each
        return remote(send.at[unit, p], readies[kind].at[j, me], send_sem.at[unit, p],
                      recv_sem.at[unit, me], rows=d)

    def own(unit):
        kind, j = unit // each, unit % each
        return pltpu.make_async_copy(send.at[unit, n - 1], readies[kind].at[j, me], own_sem.at[unit])

    for unit in range(units):
        step = units + unit
        slot = step % 2
        for copy in loads(step):
            copy.wait()

        def scaled(p, d, slot, unit):
            inverse = 1.0 / full[d, unit:unit + 1, :]
            for i in range(rows // CHUNK):
                x = wide[slot, d, i * CHUNK:(i + 1) * CHUNK, :]
                y = narrow[slot, d, i * CHUNK:(i + 1) * CHUNK, :].astype(F32)
                send[unit, p, i * CHUNK:(i + 1) * CHUNK, :] = ((x + y) * inverse).astype(BF16)

        def one(p, _, slot=slot, unit=unit):
            d = dest(p)
            scaled(p, d, slot, unit)
            data(unit, p, d).start()
            return 0

        lax.fori_loop(0, n - 1, one, 0)
        scaled(n - 1, me, slot, unit)
        own(unit).start()
        start(step + 2)

    for unit in range(units):
        kind, j = unit // each, unit % each

        def ended(k, _, unit=unit, kind=kind, j=j):
            d = (me + k) % n
            remote(send.at[unit, k - 1], readies[kind].at[j, d], send_sem.at[unit, k - 1],
                   recv_sem.at[unit, d], rows=d).wait()
            return 0

        lax.fori_loop(1, n, ended, 0)
        own(unit).wait()
    for k in range(1, owners):
        router_owners(k).wait()


def per_device(n, owners, train_gate, other_gate, train_up, other_up, router_weight, router_gain):
    experts, rows, width = train_gate.shape
    each = experts // n
    units = 2 * each
    columns = router_weight.shape[1]
    part = (router_weight * router_gain[:, None]).astype(BF16)
    lanes = 128 if rows * columns % (128 * 16) == 0 else columns
    part = part.reshape(rows * columns // lanes, lanes)
    blocks = [x.reshape(n, each, rows, width) for x in (train_gate, other_gate, train_up, other_up)]
    hbm, vmem = pl.BlockSpec(memory_space=pl.ANY), pl.BlockSpec(memory_space=pltpu.VMEM)
    ready = jax.ShapeDtypeStruct((each, n, rows, width), BF16)
    dma = pltpu.SemaphoreType.DMA
    ready_gate, ready_up, scales, router = pl.pallas_call(
        functools.partial(kernel, n, owners, each),
        out_shape=(
            ready, ready,
            jax.ShapeDtypeStruct((units, width), F32),
            jax.ShapeDtypeStruct((owners, n) + part.shape, BF16),
        ),
        in_specs=[hbm] * 4 + [vmem],
        out_specs=(hbm, hbm, vmem, hbm),
        scratch_shapes=[
            pltpu.VMEM((2, n, rows, width), F32),
            pltpu.VMEM((2, n, rows, width), BF16),
            pltpu.VMEM((units, n, rows, width), BF16),
            pltpu.VMEM((n, units, width), F32),
            pltpu.VMEM((n, units, width), F32),
            pltpu.VMEM((n, units, width), F32),
            dma((2, 2)), dma((units, n)), dma((units, n)), dma((units,)),
            dma((n,)), dma((n,)), dma((n,)), dma((n,)),
            dma((n,)), dma((n,)), dma((owners,)), dma((owners,)), dma(()),
        ],
        compiler_params=pltpu.CompilerParams(
            collective_id=0, has_side_effects=True, vmem_limit_bytes=60 * 1024 * 1024
        ),
    )(*blocks, part)
    ready_gate, ready_up = (x.reshape(each, n * rows, width) for x in (ready_gate, ready_up))
    serve_router = (
        router.reshape(owners, n * rows, columns).transpose(1, 0, 2).reshape(n * rows, owners * columns)
    )
    return (ready_gate, ready_up, scales[:each], scales[each:], serve_router)


def solution(mesh):
    n, owners = mesh.shape["rows"], mesh.shape["owner"]
    in_specs = (
        P("owner", "rows", None),
        P("owner", "rows", None),
        P("owner", "rows", None),
        P("owner", "rows", None),
        P("rows", "owner"),
        P("rows"),
    )
    out_specs = (
        P(("owner", "rows"), None, None),
        P(("owner", "rows"), None, None),
        P(("owner", "rows"), None),
        P(("owner", "rows"), None),
        P(),
    )
    return jax.shard_map(
        functools.partial(per_device, n, owners), mesh=mesh, in_specs=in_specs,
        out_specs=out_specs, check_vma=False,
    )
```
